32 devices in a mesh: dp: 2 (over y), fsdp: 16 (over z, x, core).
Axes of the slice: x: 2, y: 2, z: 4, core: 2. Of those that a mesh axis runs over, the one named last changes fastest.
Arguments:
- tokens: bfloat16 [12288, 1024], P(('dp', 'fsdp')), may hold values from -6.5 to 6.5
- cotangent: bfloat16 [12288, 1024], P(('dp', 'fsdp')), may hold values from -6 to 6
- patch_count: int32 [32], P(('dp', 'fsdp')), may hold values from 96 to 384, as said below
- image_starts: int32 [32, 8], P(('dp', 'fsdp')), may hold values from 0 to 384, as said below
- qkv_weight: bfloat16 [1024, 3072], P('fsdp'), may hold values from -8 to 8
- proj_weight: bfloat16 [1024, 1024], P('fsdp'), may hold values from -0.1875 to 0.1875
- norm_gain: bfloat16 [1024], P('fsdp'), may hold values from 0.25 to 1.75
- norm_shift: bfloat16 [1024], P('fsdp'), may hold values from -3 to 3
Outputs:
- grad_tokens: bfloat16 [12288, 1024], P(('dp', 'fsdp'))
- qkv_grad: float32 [1024, 3072], P('fsdp')
- proj_grad: float32 [1024, 1024], P('fsdp')
- gain_grad: float32 [1024], P('fsdp')
- shift_grad: float32 [1024], P('fsdp')
The draws below stay inside these ranges and needn't reach their ends.
Inputs may be any that keep to these rules, and one draw needn't show every extreme that they name: `patch_count`: at least one device has all 384 slots live; live slots of a device come first. `image_starts`: per device, non-decreasing and first 0; an image runs from its start to the next start or to the device's patch count; a start equal to the patch count marks an absent image; no image has more than 192 patches.
All inputs are finite; a program needn't handle non-finite values.
Results may differ from the reference program's by a relative error of at most 0.025.
The reference program's roundings to bfloat16 on the way count: a program that leaves them out, or rounds other values in their place, can miss the bound.
Values may be sent and summed in bfloat16 or wider, within the bound.
A program may use at most 128 MiB of HBM per device.

```python
import math
import jax
import jax.numpy as jnp
from jax import lax

D = 1024
HEAD_DIM = 64
HEADS = 16
TOK_DEV = 384
IMG_DEV = 8
TOKENS = 12288
N_DP = 2
N_FSDP = 16


def layout_draw(key):
    devices_all = N_DP * N_FSDP
    lengths = jax.random.randint(jax.random.fold_in(key, 11), (devices_all, IMG_DEV), TOK_DEV // 16 + 1, TOK_DEV // 2 + 1)
    limits = jax.random.randint(jax.random.fold_in(key, 12), (devices_all,), TOK_DEV // 4, TOK_DEV + 1)
    chosen = jax.random.randint(jax.random.fold_in(key, 13), (), 0, devices_all)
    picked = jnp.arange(devices_all, dtype=jnp.int32) == chosen
    limits = jnp.where(picked, TOK_DEV, limits)
    lengths = jnp.where(picked[:, None], TOK_DEV // 2, lengths)
    ends = jnp.cumsum(lengths, axis=1)
    starts = ends - lengths
    counts = jnp.minimum(ends[:, -1], limits).astype(jnp.int32)
    starts = jnp.minimum(starts, counts[:, None]).astype(jnp.int32)
    return (counts, starts)


def draw_patch_count(key, part):
    return layout_draw(key)[0]


def draw_image_starts(key, part):
    return layout_draw(key)[1]


def draw_tokens(key, part):
    base = jnp.clip(jax.random.normal(jax.random.fold_in(key, 21), (TOKENS, D), jnp.float32), -6.0, 6.0)
    return base.astype(jnp.bfloat16)


def draw_qkv_weight(key, part):
    base = jnp.clip(jax.random.normal(jax.random.fold_in(key, 31), (D, 3 * D), jnp.float32), -6.0, 6.0) * D ** (-0.5)
    return base.astype(jnp.bfloat16)


def block_scale(key, extent, cuts, least, top_value):
    factor_of, own = 1.0, jax.random.fold_in(key, 6)
    for axis_at, blocks in cuts:
        heights = jnp.exp(jax.random.uniform(jax.random.fold_in(own, axis_at), (blocks,), jnp.float32, least / len(cuts), top_value / len(cuts)))
        factor_of = factor_of * jnp.repeat(heights, extent[axis_at] // blocks).reshape([-1 if axis == axis_at else 1 for axis in range(len(extent))])
    return factor_of


def centred(own_key, extent, scale, limit, cuts=(), held_as=jnp.bfloat16):
    values = scale * jax.random.normal(own_key, extent, jnp.float32)
    if cuts:
        values = values * block_scale(own_key, extent, cuts, -0.22, 0.18)
    return jnp.clip(values, -limit, limit).astype(held_as)


def setup_inputs(seed: int = 0) -> dict:
    streams_of = jax.random.split(jax.random.key(seed), 9)
    return {
        "tokens": draw_tokens(jax.random.fold_in(streams_of[8], 71), 0),
        "cotangent": centred(streams_of[1], (TOKENS, D), 1.0, 6.0, ((0, 32),)),
        "patch_count": draw_patch_count(jax.random.fold_in(streams_of[8], 71), 0),
        "image_starts": draw_image_starts(jax.random.fold_in(streams_of[8], 71), 0),
        "qkv_weight": draw_qkv_weight(jax.random.fold_in(streams_of[8], 71), 0),
        "proj_weight": centred(streams_of[5], (D, D), D ** -0.5, 0.1875, ((0, 16),)),
        "norm_gain": jnp.clip(1.0 + 0.15 * jax.random.normal(streams_of[6], (D,), jnp.float32), 0.25, 1.75).astype(jnp.bfloat16),
        "norm_shift": centred(streams_of[7], (D,), 0.5, 3.0, ((0, 16),)),
    }


norm_eps = 1e-06
masked_score = -1e+30

def block_backward(block_tokens, block_cot, live_count, starts, qkv_weight, proj_weight, norm_gain, norm_shift):
    rows = block_tokens.shape[0]
    factor = HEAD_DIM ** (-0.5)
    position = jnp.arange(rows, dtype=jnp.int32)
    live = position < live_count
    segment = lax.optimization_barrier(jnp.sum((starts[None, :] <= position[:, None]).astype(jnp.int32), axis=1))
    allowed = live[:, None] & live[None, :] & (segment[:, None] == segment[None, :])
    source = block_tokens.astype(jnp.float32)
    center = lax.optimization_barrier(jnp.mean(source, axis=1, keepdims=True))
    centered = source - center
    variance = lax.optimization_barrier(jnp.mean(centered * centered, axis=1, keepdims=True))
    inverse = lax.rsqrt(variance + norm_eps)
    normed = centered * inverse
    gain = norm_gain.astype(jnp.float32)
    hidden = (normed * gain + norm_shift.astype(jnp.float32)).astype(jnp.bfloat16)
    qkv = jnp.dot(hidden, qkv_weight, preferred_element_type=jnp.float32).astype(jnp.bfloat16)
    split = qkv.reshape(rows, 3, HEADS, HEAD_DIM)
    queries = split[:, 0].astype(jnp.float32)
    keys = split[:, 1].astype(jnp.float32)
    values = split[:, 2].astype(jnp.float32)
    scores = jnp.einsum('qhe,khe->hqk', queries, keys) * factor
    scores = jnp.where(allowed[None], scores, masked_score)
    row_max = lax.optimization_barrier(jnp.max(scores, axis=2, keepdims=True))
    expon = jnp.exp(scores - row_max)
    probs = expon / lax.optimization_barrier(jnp.sum(expon, axis=2, keepdims=True))
    probs_low = probs.astype(jnp.bfloat16).astype(jnp.float32)
    attended = jnp.einsum('hqk,khe->qhe', probs_low, values).reshape(rows, D).astype(jnp.bfloat16)
    masked_cot = jnp.where(live[:, None], block_cot, jnp.zeros_like(block_cot))
    proj_term = jnp.dot(attended.T, masked_cot, preferred_element_type=jnp.float32)
    grad_attended = jnp.dot(masked_cot, proj_weight.T, preferred_element_type=jnp.float32).astype(jnp.bfloat16)
    grad_heads = grad_attended.reshape(rows, HEADS, HEAD_DIM).astype(jnp.float32)
    grad_probs = jnp.einsum('qhe,khe->hqk', grad_heads, values)
    grad_values = jnp.einsum('hqk,qhe->khe', probs_low, grad_heads).astype(jnp.bfloat16)
    grad_scores = probs * (grad_probs - lax.optimization_barrier(jnp.sum(probs * grad_probs, axis=2, keepdims=True))) * factor
    grad_scores = grad_scores.astype(jnp.bfloat16).astype(jnp.float32)
    grad_queries = jnp.einsum('hqk,khe->qhe', grad_scores, keys).astype(jnp.bfloat16)
    grad_keys = jnp.einsum('hqk,qhe->khe', grad_scores, queries).astype(jnp.bfloat16)
    grad_qkv = jnp.stack([grad_queries, grad_keys, grad_values], axis=1).reshape(rows, 3 * D)
    qkv_term = jnp.dot(hidden.T, grad_qkv, preferred_element_type=jnp.float32)
    grad_hidden = jnp.dot(grad_qkv, qkv_weight.T, preferred_element_type=jnp.float32)
    gain_term = lax.optimization_barrier(jnp.sum(grad_hidden * normed, axis=0))
    shift_term = lax.optimization_barrier(jnp.sum(grad_hidden, axis=0))
    grad_normed = grad_hidden * gain
    inner = grad_normed - lax.optimization_barrier(jnp.mean(grad_normed, axis=1, keepdims=True))
    inner = inner - normed * lax.optimization_barrier(jnp.mean(grad_normed * normed, axis=1, keepdims=True))
    grad_block = (block_cot.astype(jnp.float32) + inverse * inner).astype(jnp.bfloat16)
    return (grad_block, qkv_term, proj_term, gain_term, shift_term)

def reference(tokens, cotangent, patch_count, image_starts, qkv_weight, proj_weight, norm_gain, norm_shift):
    device_count = patch_count.shape[0]
    token_blocks = tokens.reshape(device_count, TOK_DEV, D)
    cot_blocks = cotangent.reshape(device_count, TOK_DEV, D)

    def visit(totals, inputs):
        block_tokens, block_cot, live_count, starts = inputs
        grad_block, qkv_term, proj_term, gain_term, shift_term = block_backward(block_tokens, block_cot, live_count, starts, qkv_weight, proj_weight, norm_gain, norm_shift)
        totals = (totals[0] + qkv_term, totals[1] + proj_term, totals[2] + gain_term, totals[3] + shift_term)
        return (totals, grad_block)
    start_totals = (jnp.zeros((D, 3 * D), jnp.float32), jnp.zeros((D, D), jnp.float32), jnp.zeros((D,), jnp.float32), jnp.zeros((D,), jnp.float32))
    totals, grad_blocks = lax.scan(visit, start_totals, (token_blocks, cot_blocks, patch_count, image_starts))
    factor = 1.0 / math.sqrt(TOKENS)
    return (grad_blocks.reshape(TOKENS, D), totals[0] * factor, totals[1] * factor, totals[2] * factor, totals[3] * factor)
```

```python
import functools
import math

import jax
import jax.numpy as jnp
from jax import lax
from jax.experimental import pallas as pl
from jax.experimental.pallas import tpu as pltpu
from jax.sharding import PartitionSpec as P

D = 1024
HEAD_DIM = 64
HEADS = 16


norm_eps = 1e-06
masked_score = -1e30


def block_backward(
    block_tokens, block_cot, live_count, starts, qkv_weight, proj_weight, norm_gain, norm_shift
):
    rows = block_tokens.shape[0]
    factor = HEAD_DIM ** (-0.5)
    position = jnp.arange(rows, dtype=jnp.int32)
    live = position < live_count
    segment = jnp.sum((starts[None, :] <= position[:, None]).astype(jnp.int32), axis=1)
    allowed = live[:, None] & live[None, :] & (segment[:, None] == segment[None, :])
    source = block_tokens.astype(jnp.float32)
    center = jnp.mean(source, axis=1, keepdims=True)
    centered = source - center
    variance = jnp.mean(centered * centered, axis=1, keepdims=True)
    inverse = lax.rsqrt(variance + norm_eps)
    normed = centered * inverse
    gain = norm_gain.astype(jnp.float32)
    hidden = (normed * gain + norm_shift.astype(jnp.float32)).astype(jnp.bfloat16)
    qkv = jnp.dot(hidden, qkv_weight, preferred_element_type=jnp.float32).astype(jnp.bfloat16)
    split = qkv.reshape(rows, 3, HEADS, HEAD_DIM)
    queries = split[:, 0]
    keys = split[:, 1]
    values = split[:, 2]
    scores = jnp.einsum("qhe,khe->hqk", queries, keys, preferred_element_type=jnp.float32) * factor
    scores = jnp.where(allowed[None], scores, masked_score)
    row_max = jnp.max(scores, axis=2, keepdims=True)
    expon = jnp.exp(scores - row_max)
    probs = expon / jnp.sum(expon, axis=2, keepdims=True)
    probs_low = probs.astype(jnp.bfloat16)
    attended = (
        jnp.einsum("hqk,khe->qhe", probs_low, values, preferred_element_type=jnp.float32)
        .reshape(rows, D)
        .astype(jnp.bfloat16)
    )
    masked_cot = jnp.where(live[:, None], block_cot, jnp.zeros_like(block_cot))
    proj_term = jnp.dot(attended.T, masked_cot, preferred_element_type=jnp.float32)
    grad_attended = jnp.dot(masked_cot, proj_weight.T, preferred_element_type=jnp.float32).astype(
        jnp.bfloat16
    )
    grad_heads = grad_attended.reshape(rows, HEADS, HEAD_DIM)
    grad_probs = jnp.einsum("qhe,khe->hqk", grad_heads, values, preferred_element_type=jnp.float32)
    grad_values = jnp.einsum(
        "hqk,qhe->khe", probs_low, grad_heads, preferred_element_type=jnp.float32
    ).astype(jnp.bfloat16)
    grad_scores = probs * (grad_probs - jnp.sum(probs * grad_probs, axis=2, keepdims=True)) * factor
    grad_scores = grad_scores.astype(jnp.bfloat16)
    grad_queries = jnp.einsum(
        "hqk,khe->qhe", grad_scores, keys, preferred_element_type=jnp.float32
    ).astype(jnp.bfloat16)
    grad_keys = jnp.einsum(
        "hqk,qhe->khe", grad_scores, queries, preferred_element_type=jnp.float32
    ).astype(jnp.bfloat16)
    grad_qkv = jnp.stack([grad_queries, grad_keys, grad_values], axis=1).reshape(rows, 3 * D)
    qkv_term = jnp.dot(hidden.T, grad_qkv, preferred_element_type=jnp.float32)
    grad_hidden = jnp.dot(grad_qkv, qkv_weight.T, preferred_element_type=jnp.float32)
    gain_term = jnp.sum(grad_hidden * normed, axis=0)
    shift_term = jnp.sum(grad_hidden, axis=0)
    grad_normed = grad_hidden * gain
    inner = grad_normed - jnp.mean(grad_normed, axis=1, keepdims=True)
    inner = inner - normed * jnp.mean(grad_normed * normed, axis=1, keepdims=True)
    grad_block = (block_cot.astype(jnp.float32) + inverse * inner).astype(jnp.bfloat16)
    return (grad_block, qkv_term, proj_term, gain_term, shift_term)


LANES = 128
CORES = 2
LONG = 4


def grid_of(owners):
    long_size = LONG if owners % (LONG * CORES) == 0 else 1
    return long_size, owners // (long_size * CORES)


def inside(at, size):
    return jnp.logical_and(at >= 0, at < size)


def place(owners):
    long_size, across_size = grid_of(owners)
    me = lax.axis_index("fsdp")
    core = lax.rem(me, CORES)
    across = lax.rem(lax.div(me, CORES), across_size)
    along = lax.div(me, CORES * across_size)
    return me, along, across, core


def neighbours(owners):
    long_size, across_size = grid_of(owners)
    me, along, across, core = place(owners)
    return (
        (along + 1 < long_size, me + CORES * across_size),
        (along >= 1, me - CORES * across_size),
        (across + 1 < across_size, me + CORES),
        (across >= 1, me - CORES),
        (core >= 0, me + 1 - 2 * core),
    )


def greet(owners, replicas):
    barrier = pltpu.get_barrier_semaphore()
    count = jnp.int32(0)
    for there, target in neighbours(owners):
        count = count + there.astype(jnp.int32)

        @pl.when(there)
        def _():
            pl.semaphore_signal(barrier, inc=1, device_id={"fsdp": target})

    mine = lax.axis_index("dp")
    for step in range(1, replicas):
        pl.semaphore_signal(
            barrier, inc=1, device_id={"dp": lax.rem(mine + step, replicas)}
        )
    pl.semaphore_wait(barrier, count + (replicas - 1))


def gather_kernel(owners, own_ref, qkv_ref, proj_ref, small_ref, held, send_sem, recv_sem):
    long_size, across_size = grid_of(owners)
    me, along, across, core = place(owners)
    rows = own_ref.shape[0]
    width = qkv_ref.shape[1]
    square = proj_ref.shape[1]
    greet(owners, 1)
    steps = [(0, 0)]
    for total in range(1, long_size + across_size - 1):
        for far in range(min(total, long_size - 1), -1, -1):
            side = total - far
            if side >= across_size:
                continue
            for up in (1, -1) if far else (1,):
                for out in (1, -1) if side else (1,):
                    steps.append((up * far, out * side))

    def copies(up, out):
        at_long, at_across = along + up, across + out
        piece = (at_long * across_size + at_across) * CORES + core
        source = own_ref if up == 0 and out == 0 else held.at[piece]
        there = neighbours(owners)
        use = [out == 0 and up <= 0, out == 0 and up >= 0, out <= 0, out >= 0, True]
        made = []
        for way in range(5):
            if use[way]:
                copy = pltpu.make_async_remote_copy(
                    src_ref=source,
                    dst_ref=held.at[piece],
                    send_sem=send_sem.at[way, piece],
                    recv_sem=recv_sem.at[piece],
                    device_id={"fsdp": there[way][1]},
                )
                made.append((there[way][0], copy))
        there_is = jnp.logical_and(inside(at_long, long_size), inside(at_across, across_size))
        return piece, there_is, made

    def arrived(piece):
        pltpu.make_async_remote_copy(
            src_ref=own_ref,
            dst_ref=held.at[piece],
            send_sem=send_sem.at[0, piece],
            recv_sem=recv_sem.at[piece],
            device_id={"fsdp": me + 1 - 2 * core},
        ).wait_recv()

    for up, out in steps:
        piece, there_is, made = copies(up, out)

        @pl.when(there_is)
        def _():
            if up != 0 or out != 0:
                arrived(piece)
            for exists, copy in made:
                @pl.when(exists)
                def _():
                    copy.start()

    qkv_ref[pl.ds(pl.multiple_of(me * rows, rows), rows), :] = own_ref[:, :width]
    proj_ref[pl.ds(pl.multiple_of(me * rows, rows), rows), :] = own_ref[:, width : width + square]
    small_ref[me] = own_ref[:, width + square :]

    def unpack(pair, carry):
        piece = pair * CORES + 1 - core
        arrived(piece)
        for one in range(CORES):
            at = pair * CORES + one

            @pl.when(at != me)
            def _():
                start = pl.ds(pl.multiple_of(at * rows, rows), rows)
                qkv_ref[start, :] = held[at, :, :width]
                proj_ref[start, :] = held[at, :, width : width + square]
                small_ref[at] = held[at, :, width + square :]

        return carry

    lax.fori_loop(0, owners // CORES, unpack, 0)
    for up, out in steps:
        piece, there_is, made = copies(up, out)

        @pl.when(there_is)
        def _():
            for exists, copy in made:
                @pl.when(exists)
                def _():
                    copy.wait_send()


def gather_all(owners, own, width, square):
    rows, packed = own.shape
    return pl.pallas_call(
        functools.partial(gather_kernel, owners),
        name="gather_all",
        out_shape=(
            jax.ShapeDtypeStruct((owners * rows, width), jnp.bfloat16),
            jax.ShapeDtypeStruct((owners * rows, square), jnp.bfloat16),
            jax.ShapeDtypeStruct((owners, rows, LANES), jnp.bfloat16),
        ),
        in_specs=[pl.BlockSpec(memory_space=pltpu.VMEM)],
        out_specs=(pl.BlockSpec(memory_space=pltpu.VMEM),) * 3,
        scratch_shapes=[
            pltpu.VMEM((owners, rows, packed), jnp.bfloat16),
            pltpu.SemaphoreType.DMA((5, owners)),
            pltpu.SemaphoreType.DMA((owners,)),
        ],
        compiler_params=pltpu.CompilerParams(
            collective_id=0, has_side_effects=True, vmem_limit_bytes=48 * 2**20
        ),
    )(own)


def scatter_kernel(
    owners, replicas, factor,
    qkv_ref, proj_ref, small_ref, qkv_out, proj_out, small_out,
    from_qkv, from_proj, from_small, part, from_left, from_right, line, from_low, from_high,
    mine_ref, twins, core_send, core_recv, across_send, across_recv, long_send, long_recv,
    twin_send, twin_recv,
):
    long_size, across_size = grid_of(owners)
    me, along, across, core = place(owners)
    rows = qkv_out.shape[0]
    width = qkv_out.shape[1]
    square = proj_out.shape[1]
    pairs = owners // CORES
    wide = jnp.float32
    low = jnp.bfloat16
    greet(owners, replicas)
    sibling = {"fsdp": me + 1 - 2 * core}

    order = [
        (step_long, step_across)
        for step_long in range(long_size)
        for step_across in range(across_size)
    ]

    def spot(step_long, step_across):
        at_long = lax.rem(along + 1 + step_long, long_size)
        at_across = lax.rem(across + 1 + step_across, across_size)
        return at_long, at_across

    def core_copies(at_long, at_across):
        pair = at_long * across_size + at_across
        block = pair * CORES + 1 - core
        start = pl.ds(pl.multiple_of(block * rows, rows), rows)
        made = []
        for kind, (src, dst) in enumerate(
            (
                (qkv_ref.at[start, :], from_qkv.at[pair]),
                (proj_ref.at[start, :], from_proj.at[pair]),
                (small_ref.at[block], from_small.at[pair]),
            )
        ):
            made.append(
                pltpu.make_async_remote_copy(
                    src_ref=src,
                    dst_ref=dst,
                    send_sem=core_send.at[kind, pair],
                    recv_sem=core_recv.at[kind, pair],
                    device_id=sibling,
                )
            )
        return made

    for steps in order:
        for copy in core_copies(*spot(*steps)):
            copy.start()

    def across_copy(at_long, at_across, way):
        pair = at_long * across_size + at_across
        landing = from_left if way > 0 else from_right
        side = 0 if way > 0 else 1
        return pltpu.make_async_remote_copy(
            src_ref=part.at[pair],
            dst_ref=landing.at[pair],
            send_sem=across_send.at[side, pair],
            recv_sem=across_recv.at[side, pair],
            device_id={"fsdp": me + way * CORES},
        )

    def long_copy(at_long, way):
        landing = from_low if way > 0 else from_high
        side = 0 if way > 0 else 1
        return pltpu.make_async_remote_copy(
            src_ref=line.at[at_long],
            dst_ref=landing.at[at_long],
            send_sem=long_send.at[side, at_long],
            recv_sem=long_recv.at[side, at_long],
            device_id={"fsdp": me + way * CORES * across_size},
        )

    for steps in order:
        at_long, at_across = spot(*steps)
        pair = at_long * across_size + at_across
        for copy in core_copies(at_long, at_across):
            copy.wait_recv()
        block = pair * CORES + core
        start = pl.ds(pl.multiple_of(block * rows, rows), rows)
        part[pair, :, :width] = (qkv_ref[start, :].astype(wide) + from_qkv[pair].astype(wide)).astype(low)
        part[pair, :, width : width + square] = (
            proj_ref[start, :].astype(wide) + from_proj[pair].astype(wide)
        ).astype(low)
        part[pair, :, width + square :] = (
            small_ref[block].astype(wide) + from_small[pair].astype(wide)
        ).astype(low)

        if steps[1] < across_size - 1:
            for way in (1, -1):
                @pl.when((at_across - across) * way > 0)
                def _():
                    @pl.when(inside(across - way, across_size))
                    def _():
                        across_copy(at_long, at_across, way).wait_recv()
                        landing = from_left if way > 0 else from_right
                        part[pair] = (part[pair].astype(wide) + landing[pair].astype(wide)).astype(low)

                    across_copy(at_long, at_across, way).start()

    for step_long in range(long_size):
        at_long = lax.rem(along + 1 + step_long, long_size)
        pair = at_long * across_size + across
        line[at_long] = part[pair]
        for way in (1, -1):
            @pl.when(inside(across - way, across_size))
            def _():
                across_copy(at_long, across, way).wait_recv()
                landing = from_left if way > 0 else from_right
                line[at_long] = (line[at_long].astype(wide) + landing[pair].astype(wide)).astype(low)

        for way in (1, -1):
            @pl.when(inside(along - way, long_size))
            def _():
                @pl.when((at_long - along) * way >= 0)
                def _():
                    long_copy(at_long, way).wait_recv()
                    landing = from_low if way > 0 else from_high
                    line[at_long] = (line[at_long].astype(wide) + landing[at_long].astype(wide)).astype(low)

            @pl.when((at_long - along) * way > 0)
            def _():
                long_copy(at_long, way).start()

    mine_ref[...] = line[along]
    twin = lax.axis_index("dp")

    def twin_copy(step):
        return pltpu.make_async_remote_copy(
            src_ref=mine_ref,
            dst_ref=twins.at[step],
            send_sem=twin_send.at[step],
            recv_sem=twin_recv.at[step],
            device_id={"dp": lax.rem(twin + step, replicas)},
        )

    for step in range(1, replicas):
        twin_copy(step).start()
    for step in range(1, replicas):
        twin_copy(step).wait()
    twins[0] = mine_ref[...]
    total = jnp.zeros(mine_ref.shape, wide)
    for rank in range(replicas):
        total = total + twins[lax.rem(twin - rank + replicas, replicas)].astype(wide)
    total = total * factor
    qkv_out[...] = total[:, :width]
    proj_out[...] = total[:, width : width + square]
    small_out[...] = total[:, width + square :]

    for steps in order:
        at_long, at_across = spot(*steps)
        for copy in core_copies(at_long, at_across):
            copy.wait_send()
        if steps[1] < across_size - 1:
            for way in (1, -1):
                @pl.when((at_across - across) * way > 0)
                def _():
                    across_copy(at_long, at_across, way).wait_send()

    for step_long in range(long_size):
        at_long = lax.rem(along + 1 + step_long, long_size)
        for way in (1, -1):
            @pl.when((at_long - along) * way > 0)
            def _():
                long_copy(at_long, way).wait_send()


def scatter_all(owners, replicas, factor, qkv_term, proj_term, small):
    long_size, across_size = grid_of(owners)
    pairs = owners // CORES
    rows = qkv_term.shape[0] // owners
    width = qkv_term.shape[1]
    square = proj_term.shape[1]
    packed = width + square + LANES
    low = jnp.bfloat16
    block = (rows, packed)
    dma = pltpu.SemaphoreType.DMA
    return pl.pallas_call(
        functools.partial(scatter_kernel, owners, replicas, factor),
        name="scatter_all",
        out_shape=(
            jax.ShapeDtypeStruct((rows, width), jnp.float32),
            jax.ShapeDtypeStruct((rows, square), jnp.float32),
            jax.ShapeDtypeStruct((rows, LANES), jnp.float32),
        ),
        in_specs=[pl.BlockSpec(memory_space=pltpu.VMEM)] * 3,
        out_specs=(pl.BlockSpec(memory_space=pltpu.VMEM),) * 3,
        scratch_shapes=[
            pltpu.VMEM((pairs, rows, width), low),
            pltpu.VMEM((pairs, rows, square), low),
            pltpu.VMEM((pairs, rows, LANES), low),
            pltpu.VMEM((pairs,) + block, low),
            pltpu.VMEM((pairs,) + block, low),
            pltpu.VMEM((pairs,) + block, low),
            pltpu.VMEM((long_size,) + block, low),
            pltpu.VMEM((long_size,) + block, low),
            pltpu.VMEM((long_size,) + block, low),
            pltpu.VMEM(block, low),
            pltpu.VMEM((replicas,) + block, low),
            dma((3, pairs)),
            dma((3, pairs)),
            dma((2, pairs)),
            dma((2, pairs)),
            dma((2, long_size)),
            dma((2, long_size)),
            dma((replicas,)),
            dma((replicas,)),
        ],
        compiler_params=pltpu.CompilerParams(
            collective_id=1, has_side_effects=True, vmem_limit_bytes=60 * 2**20
        ),
    )(qkv_term, proj_term, small)


def per_device(
    tokens, cotangent, patch_count, image_starts, qkv_weight, proj_weight, norm_gain, norm_shift
):
    replicas = lax.axis_size("dp")
    owners = lax.axis_size("fsdp")
    rows, width = qkv_weight.shape
    square = proj_weight.shape[1]
    model = owners * rows
    own_small = jnp.stack([norm_gain, norm_shift], axis=1)
    own_small = jnp.pad(own_small, ((0, 0), (0, LANES - 2)))
    own = jnp.concatenate([qkv_weight, proj_weight, own_small], axis=1)
    whole_qkv, whole_proj, whole_small = gather_all(owners, own, width, square)
    whole_small = whole_small[:, :, :2].reshape(model, 2)
    grad_block, qkv_term, proj_term, gain_term, shift_term = block_backward(
        tokens,
        cotangent,
        patch_count[0],
        image_starts[0],
        whole_qkv,
        whole_proj,
        whole_small[:, 0],
        whole_small[:, 1],
    )
    factor = 1.0 / math.sqrt(tokens.shape[0] * replicas * owners)
    small = jnp.stack([gain_term, shift_term], axis=1).astype(jnp.bfloat16)
    small = jnp.pad(small, ((0, 0), (0, LANES - 2))).reshape(owners, rows, LANES)
    qkv_grad, proj_grad, small_grad = scatter_all(
        owners,
        replicas,
        factor,
        qkv_term.astype(jnp.bfloat16),
        proj_term.astype(jnp.bfloat16),
        small,
    )
    return (grad_block, qkv_grad, proj_grad, small_grad[:, 0], small_grad[:, 1])


def solution(mesh):
    placed = (
        P(("dp", "fsdp"), None),
        P(("dp", "fsdp"), None),
        P(("dp", "fsdp")),
        P(("dp", "fsdp"), None),
        P("fsdp", None),
        P("fsdp", None),
        P("fsdp"),
        P("fsdp"),
    )
    return jax.shard_map(
        per_device,
        mesh=mesh,
        in_specs=placed,
        out_specs=(P(("dp", "fsdp"), None), P("fsdp", None), P("fsdp", None), P("fsdp"), P("fsdp")),
        check_vma=False,
    )
```

```python
import functools
import math

import jax
import jax.numpy as jnp
from jax import lax
from jax.experimental import pallas as pl
from jax.experimental.pallas import tpu as pltpu
from jax.sharding import PartitionSpec as P

D = 1024
HEAD_DIM = 64
HEADS = 16


norm_eps = 1e-06
masked_score = -1e30


def dot_rows(a, b):
    return lax.dot_general(a, b, (((1,), (1,)), ((), ())), preferred_element_type=jnp.float32)


def dot_cols(a, b):
    return lax.dot_general(a, b, (((0,), (0,)), ((), ())), preferred_element_type=jnp.float32)


def attention_kernel(by_row, by_col, q_ref, k_ref, v_ref, g_ref, attended_ref, grad_ref):
    at = pl.program_id(0)
    heads = q_ref.shape[1] // HEAD_DIM
    rows, lanes = q_ref.shape
    model = attended_ref.shape[1] * pl.num_programs(0)
    factor = HEAD_DIM ** (-0.5)
    allowed = (by_row[...] == by_col[...]) & (by_row[...] >= 0)
    head_of = lax.broadcasted_iota(jnp.int32, (1, lanes), 1) // HEAD_DIM
    q, k, v, g = q_ref[...], k_ref[...], v_ref[...], g_ref[...]
    sums = [jnp.zeros((rows, lanes), jnp.float32)] * 4
    for head in range(heads):
        mask = (head_of == head).astype(jnp.float32).astype(jnp.bfloat16)
        q_own, k_own, v_own, g_own = q * mask, k * mask, v * mask, g * mask
        scores = jnp.where(allowed, dot_rows(q_own, k) * factor, masked_score)
        expon = jnp.exp(scores - jnp.max(scores, axis=1, keepdims=True))
        probs = expon * (1.0 / jnp.sum(expon, axis=1, keepdims=True))
        probs_low = probs.astype(jnp.bfloat16)
        grad_probs = dot_rows(g_own, v)
        inner = jnp.sum(probs * grad_probs, axis=1, keepdims=True)
        grad_scores = (probs * (grad_probs - inner) * factor).astype(jnp.bfloat16)
        terms = (
            jnp.dot(probs_low, v_own, preferred_element_type=jnp.float32),
            jnp.dot(grad_scores, k_own, preferred_element_type=jnp.float32),
            dot_cols(grad_scores, q_own),
            dot_cols(probs_low, g_own),
        )
        sums = [a + b for a, b in zip(sums, terms)]
    attended_ref[...] = sums[0].astype(jnp.bfloat16)
    for kind in range(3):
        start = pl.multiple_of(kind * model + at * lanes, lanes)
        grad_ref[:, pl.ds(start, lanes)] = sums[kind + 1].astype(jnp.bfloat16)


def attention(qkv, grad_attended, marks):
    rows, model = grad_attended.shape
    lanes = 2 * HEAD_DIM
    steps = model // lanes
    spec = lambda shift: pl.BlockSpec((rows, lanes), lambda i: (0, shift * steps + i))
    return pl.pallas_call(
        attention_kernel,
        name="attention",
        grid=(steps,),
        out_shape=(
            jax.ShapeDtypeStruct((rows, model), jnp.bfloat16),
            jax.ShapeDtypeStruct((rows, 3 * model), jnp.bfloat16),
        ),
        in_specs=[
            pl.BlockSpec((rows, 1), lambda i: (0, 0)),
            pl.BlockSpec((1, rows), lambda i: (0, 0)),
            spec(0),
            spec(1),
            spec(2),
            spec(0),
        ],
        out_specs=(spec(0), pl.BlockSpec((rows, 3 * model), lambda i: (0, 0))),
        compiler_params=pltpu.CompilerParams(vmem_limit_bytes=40 * 2**20),
    )(marks[:, None], marks[None, :], qkv, qkv, qkv, grad_attended)


def block_backward(
    block_tokens, block_cot, live_count, starts, qkv_weight, proj_weight, norm_gain, norm_shift
):
    rows = block_tokens.shape[0]
    position = jnp.arange(rows, dtype=jnp.int32)
    live = position < live_count
    segment = jnp.sum((starts[None, :] <= position[:, None]).astype(jnp.int32), axis=1)
    source = block_tokens.astype(jnp.float32)
    center = jnp.mean(source, axis=1, keepdims=True)
    centered = source - center
    variance = jnp.mean(centered * centered, axis=1, keepdims=True)
    inverse = lax.rsqrt(variance + norm_eps)
    normed = centered * inverse
    gain = norm_gain.astype(jnp.float32)
    hidden = (normed * gain + norm_shift.astype(jnp.float32)).astype(jnp.bfloat16)
    qkv = jnp.dot(hidden, qkv_weight, preferred_element_type=jnp.float32).astype(jnp.bfloat16)
    masked_cot = jnp.where(live[:, None], block_cot, jnp.zeros_like(block_cot))
    grad_attended = jnp.dot(masked_cot, proj_weight.T, preferred_element_type=jnp.float32).astype(
        jnp.bfloat16
    )
    attended, grad_qkv = attention(qkv, grad_attended, jnp.where(live, segment, -1))
    proj_term = jnp.dot(attended.T, masked_cot, preferred_element_type=jnp.float32)
    qkv_term = jnp.dot(hidden.T, grad_qkv, preferred_element_type=jnp.float32)
    grad_hidden = jnp.dot(grad_qkv, qkv_weight.T, preferred_element_type=jnp.float32)
    gain_term = jnp.sum(grad_hidden * normed, axis=0)
    shift_term = jnp.sum(grad_hidden, axis=0)
    grad_normed = grad_hidden * gain
    inner = grad_normed - jnp.mean(grad_normed, axis=1, keepdims=True)
    inner = inner - normed * jnp.mean(grad_normed * normed, axis=1, keepdims=True)
    grad_block = (block_cot.astype(jnp.float32) + inverse * inner).astype(jnp.bfloat16)
    return (grad_block, qkv_term, proj_term, gain_term, shift_term)


LANES = 128
CORES = 2
LONG = 4


def grid_of(owners):
    long_size = LONG if owners % (LONG * CORES) == 0 else 1
    return long_size, owners // (long_size * CORES)


def inside(at, size):
    return jnp.logical_and(at >= 0, at < size)


def place(owners):
    long_size, across_size = grid_of(owners)
    me = lax.axis_index("fsdp")
    core = lax.rem(me, CORES)
    across = lax.rem(lax.div(me, CORES), across_size)
    along = lax.div(me, CORES * across_size)
    return me, along, across, core


def neighbours(owners):
    long_size, across_size = grid_of(owners)
    me, along, across, core = place(owners)
    return (
        (along + 1 < long_size, me + CORES * across_size),
        (along >= 1, me - CORES * across_size),
        (across + 1 < across_size, me + CORES),
        (across >= 1, me - CORES),
        (core >= 0, me + 1 - 2 * core),
    )


def greet(owners, replicas):
    barrier = pltpu.get_barrier_semaphore()
    count = jnp.int32(0)
    for there, target in neighbours(owners):
        count = count + there.astype(jnp.int32)

        @pl.when(there)
        def _():
            pl.semaphore_signal(barrier, inc=1, device_id={"fsdp": target})

    mine = lax.axis_index("dp")
    for step in range(1, replicas):
        pl.semaphore_signal(
            barrier, inc=1, device_id={"dp": lax.rem(mine + step, replicas)}
        )
    pl.semaphore_wait(barrier, count + (replicas - 1))


def gather_kernel(owners, own_ref, qkv_ref, proj_ref, small_ref, held, send_sem, recv_sem):
    long_size, across_size = grid_of(owners)
    me, along, across, core = place(owners)
    rows = own_ref.shape[0]
    width = qkv_ref.shape[1]
    square = proj_ref.shape[1]
    greet(owners, 1)
    steps = [(0, 0)]
    for total in range(1, long_size + across_size - 1):
        for far in range(min(total, long_size - 1), -1, -1):
            side = total - far
            if side >= across_size:
                continue
            for up in (1, -1) if far else (1,):
                for out in (1, -1) if side else (1,):
                    steps.append((up * far, out * side))

    def copies(up, out):
        at_long, at_across = along + up, across + out
        piece = (at_long * across_size + at_across) * CORES + core
        source = own_ref if up == 0 and out == 0 else held.at[piece]
        there = neighbours(owners)
        use = [out == 0 and up <= 0, out == 0 and up >= 0, out <= 0, out >= 0, True]
        made = []
        for way in range(5):
            if use[way]:
                copy = pltpu.make_async_remote_copy(
                    src_ref=source,
                    dst_ref=held.at[piece],
                    send_sem=send_sem.at[way, piece],
                    recv_sem=recv_sem.at[piece],
                    device_id={"fsdp": there[way][1]},
                )
                made.append((there[way][0], copy))
        there_is = jnp.logical_and(inside(at_long, long_size), inside(at_across, across_size))
        return piece, there_is, made

    def arrived(piece):
        pltpu.make_async_remote_copy(
            src_ref=own_ref,
            dst_ref=held.at[piece],
            send_sem=send_sem.at[0, piece],
            recv_sem=recv_sem.at[piece],
            device_id={"fsdp": me + 1 - 2 * core},
        ).wait_recv()

    for up, out in steps:
        piece, there_is, made = copies(up, out)

        @pl.when(there_is)
        def _():
            if up != 0 or out != 0:
                arrived(piece)
            for exists, copy in made:
                @pl.when(exists)
                def _():
                    copy.start()

    qkv_ref[pl.ds(pl.multiple_of(me * rows, rows), rows), :] = own_ref[:, :width]
    proj_ref[pl.ds(pl.multiple_of(me * rows, rows), rows), :] = own_ref[:, width : width + square]
    small_ref[me] = own_ref[:, width + square :]

    def unpack(pair, carry):
        piece = pair * CORES + 1 - core
        arrived(piece)
        for one in range(CORES):
            at = pair * CORES + one

            @pl.when(at != me)
            def _():
                start = pl.ds(pl.multiple_of(at * rows, rows), rows)
                qkv_ref[start, :] = held[at, :, :width]
                proj_ref[start, :] = held[at, :, width : width + square]
                small_ref[at] = held[at, :, width + square :]

        return carry

    lax.fori_loop(0, owners // CORES, unpack, 0)
    for up, out in steps:
        piece, there_is, made = copies(up, out)

        @pl.when(there_is)
        def _():
            for exists, copy in made:
                @pl.when(exists)
                def _():
                    copy.wait_send()


def gather_all(owners, own, width, square):
    rows, packed = own.shape
    return pl.pallas_call(
        functools.partial(gather_kernel, owners),
        name="gather_all",
        out_shape=(
            jax.ShapeDtypeStruct((owners * rows, width), jnp.bfloat16),
            jax.ShapeDtypeStruct((owners * rows, square), jnp.bfloat16),
            jax.ShapeDtypeStruct((owners, rows, LANES), jnp.bfloat16),
        ),
        in_specs=[pl.BlockSpec(memory_space=pltpu.VMEM)],
        out_specs=(pl.BlockSpec(memory_space=pltpu.VMEM),) * 3,
        scratch_shapes=[
            pltpu.VMEM((owners, rows, packed), jnp.bfloat16),
            pltpu.SemaphoreType.DMA((5, owners)),
            pltpu.SemaphoreType.DMA((owners,)),
        ],
        compiler_params=pltpu.CompilerParams(
            collective_id=0, has_side_effects=True, vmem_limit_bytes=48 * 2**20
        ),
    )(own)


def scatter_kernel(
    owners, replicas, factor,
    qkv_ref, proj_ref, small_ref, qkv_out, proj_out, small_out,
    from_qkv, from_proj, from_small, part, from_left, from_right, line, from_low, from_high,
    mine_ref, twins, core_send, core_recv, across_send, across_recv, long_send, long_recv,
    twin_send, twin_recv,
):
    long_size, across_size = grid_of(owners)
    me, along, across, core = place(owners)
    rows = qkv_out.shape[0]
    width = qkv_out.shape[1]
    square = proj_out.shape[1]
    wide = jnp.float32
    low = jnp.bfloat16
    greet(owners, replicas)
    sibling = {"fsdp": me + 1 - 2 * core}

    def outward(size):
        return [sign * far for far in range(size - 1, 0, -1) for sign in (1, -1)] + [0]

    order = [(up, out) for up in outward(long_size) for out in outward(across_size)]

    def spot(up, out):
        return along + up, across + out

    def there(at_long, at_across):
        return jnp.logical_and(inside(at_long, long_size), inside(at_across, across_size))

    def core_copies(at_long, at_across):
        pair = at_long * across_size + at_across
        block = pair * CORES + 1 - core
        start = pl.ds(pl.multiple_of(block * rows, rows), rows)
        made = []
        for kind, (src, dst) in enumerate(
            (
                (qkv_ref.at[start, :], from_qkv.at[pair]),
                (proj_ref.at[start, :], from_proj.at[pair]),
                (small_ref.at[block], from_small.at[pair]),
            )
        ):
            made.append(
                pltpu.make_async_remote_copy(
                    src_ref=src,
                    dst_ref=dst,
                    send_sem=core_send.at[kind, pair],
                    recv_sem=core_recv.at[kind, pair],
                    device_id=sibling,
                )
            )
        return made

    for steps in order:
        @pl.when(there(*spot(*steps)))
        def _():
            for copy in core_copies(*spot(*steps)):
                copy.start()

    def across_copy(at_long, at_across, way):
        pair = at_long * across_size + at_across
        landing = from_left if way > 0 else from_right
        side = 0 if way > 0 else 1
        return pltpu.make_async_remote_copy(
            src_ref=part.at[pair],
            dst_ref=landing.at[pair],
            send_sem=across_send.at[side, pair],
            recv_sem=across_recv.at[side, pair],
            device_id={"fsdp": me + way * CORES},
        )

    def long_copy(at_long, way):
        landing = from_low if way > 0 else from_high
        side = 0 if way > 0 else 1
        return pltpu.make_async_remote_copy(
            src_ref=line.at[at_long],
            dst_ref=landing.at[at_long],
            send_sem=long_send.at[side, at_long],
            recv_sem=long_recv.at[side, at_long],
            device_id={"fsdp": me + way * CORES * across_size},
        )

    def join(steps):
        at_long, at_across = spot(*steps)
        pair = at_long * across_size + at_across
        for copy in core_copies(at_long, at_across):
            copy.wait_recv()
        block = pair * CORES + core
        start = pl.ds(pl.multiple_of(block * rows, rows), rows)
        part[pair, :, :width] = (qkv_ref[start, :].astype(wide) + from_qkv[pair].astype(wide)).astype(low)
        part[pair, :, width : width + square] = (
            proj_ref[start, :].astype(wide) + from_proj[pair].astype(wide)
        ).astype(low)
        part[pair, :, width + square :] = (
            small_ref[block].astype(wide) + from_small[pair].astype(wide)
        ).astype(low)
        if steps[1] != 0:
            way = 1 if steps[1] > 0 else -1

            @pl.when(inside(across - way, across_size))
            def _():
                across_copy(at_long, at_across, way).wait_recv()
                landing = from_left if way > 0 else from_right
                part[pair] = (part[pair].astype(wide) + landing[pair].astype(wide)).astype(low)

            across_copy(at_long, at_across, way).start()

    for steps in order:
        @pl.when(there(*spot(*steps)))
        def _():
            join(steps)

    def settle(up):
        at_long = along + up
        pair = at_long * across_size + across
        line[at_long] = part[pair]
        for way in (1, -1):
            @pl.when(inside(across - way, across_size))
            def _():
                across_copy(at_long, across, way).wait_recv()
                landing = from_left if way > 0 else from_right
                line[at_long] = (line[at_long].astype(wide) + landing[pair].astype(wide)).astype(low)

        for way in (1, -1):
            if up * way >= 0:
                @pl.when(inside(along - way, long_size))
                def _():
                    long_copy(at_long, way).wait_recv()
                    landing = from_low if way > 0 else from_high
                    line[at_long] = (line[at_long].astype(wide) + landing[at_long].astype(wide)).astype(low)

            if up * way > 0:
                long_copy(at_long, way).start()

    for up in outward(long_size):
        @pl.when(inside(along + up, long_size))
        def _():
            settle(up)

    mine_ref[...] = line[along]
    twin = lax.axis_index("dp")

    def twin_copy(step):
        return pltpu.make_async_remote_copy(
            src_ref=mine_ref,
            dst_ref=twins.at[step],
            send_sem=twin_send.at[step],
            recv_sem=twin_recv.at[step],
            device_id={"dp": lax.rem(twin + step, replicas)},
        )

    for step in range(1, replicas):
        twin_copy(step).start()
    for step in range(1, replicas):
        twin_copy(step).wait()
    twins[0] = mine_ref[...]
    total = jnp.zeros(mine_ref.shape, wide)
    for rank in range(replicas):
        total = total + twins[lax.rem(twin - rank + replicas, replicas)].astype(wide)
    total = total * factor
    qkv_out[...] = total[:, :width]
    proj_out[...] = total[:, width : width + square]
    small_out[...] = total[:, width + square :]

    for steps in order:
        at_long, at_across = spot(*steps)

        @pl.when(there(at_long, at_across))
        def _():
            for copy in core_copies(at_long, at_across):
                copy.wait_send()
            if steps[1] != 0:
                across_copy(at_long, at_across, 1 if steps[1] > 0 else -1).wait_send()

    for up in outward(long_size):
        if up != 0:
            @pl.when(inside(along + up, long_size))
            def _():
                long_copy(along + up, 1 if up > 0 else -1).wait_send()


def scatter_all(owners, replicas, factor, qkv_term, proj_term, small):
    long_size, across_size = grid_of(owners)
    pairs = owners // CORES
    rows = qkv_term.shape[0] // owners
    width = qkv_term.shape[1]
    square = proj_term.shape[1]
    packed = width + square + LANES
    low = jnp.bfloat16
    block = (rows, packed)
    dma = pltpu.SemaphoreType.DMA
    return pl.pallas_call(
        functools.partial(scatter_kernel, owners, replicas, factor),
        name="scatter_all",
        out_shape=(
            jax.ShapeDtypeStruct((rows, width), jnp.float32),
            jax.ShapeDtypeStruct((rows, square), jnp.float32),
            jax.ShapeDtypeStruct((rows, LANES), jnp.float32),
        ),
        in_specs=[pl.BlockSpec(memory_space=pltpu.VMEM)] * 3,
        out_specs=(pl.BlockSpec(memory_space=pltpu.VMEM),) * 3,
        scratch_shapes=[
            pltpu.VMEM((pairs, rows, width), low),
            pltpu.VMEM((pairs, rows, square), low),
            pltpu.VMEM((pairs, rows, LANES), low),
            pltpu.VMEM((pairs,) + block, low),
            pltpu.VMEM((pairs,) + block, low),
            pltpu.VMEM((pairs,) + block, low),
            pltpu.VMEM((long_size,) + block, low),
            pltpu.VMEM((long_size,) + block, low),
            pltpu.VMEM((long_size,) + block, low),
            pltpu.VMEM(block, low),
            pltpu.VMEM((replicas,) + block, low),
            dma((3, pairs)),
            dma((3, pairs)),
            dma((2, pairs)),
            dma((2, pairs)),
            dma((2, long_size)),
            dma((2, long_size)),
            dma((replicas,)),
            dma((replicas,)),
        ],
        compiler_params=pltpu.CompilerParams(
            collective_id=1, has_side_effects=True, vmem_limit_bytes=60 * 2**20
        ),
    )(qkv_term, proj_term, small)


def per_device(
    tokens, cotangent, patch_count, image_starts, qkv_weight, proj_weight, norm_gain, norm_shift
):
    replicas = lax.axis_size("dp")
    owners = lax.axis_size("fsdp")
    rows, width = qkv_weight.shape
    square = proj_weight.shape[1]
    model = owners * rows
    own_small = jnp.stack([norm_gain, norm_shift], axis=1)
    own_small = jnp.pad(own_small, ((0, 0), (0, LANES - 2)))
    own = jnp.concatenate([qkv_weight, proj_weight, own_small], axis=1)
    whole_qkv, whole_proj, whole_small = gather_all(owners, own, width, square)
    whole_small = whole_small[:, :, :2].reshape(model, 2)
    grad_block, qkv_term, proj_term, gain_term, shift_term = block_backward(
        tokens,
        cotangent,
        patch_count[0],
        image_starts[0],
        whole_qkv,
        whole_proj,
        whole_small[:, 0],
        whole_small[:, 1],
    )
    factor = 1.0 / math.sqrt(tokens.shape[0] * replicas * owners)
    small = jnp.stack([gain_term, shift_term], axis=1).astype(jnp.bfloat16)
    small = jnp.pad(small, ((0, 0), (0, LANES - 2))).reshape(owners, rows, LANES)
    qkv_grad, proj_grad, small_grad = scatter_all(
        owners,
        replicas,
        factor,
        qkv_term.astype(jnp.bfloat16),
        proj_term.astype(jnp.bfloat16),
        small,
    )
    return (grad_block, qkv_grad, proj_grad, small_grad[:, 0], small_grad[:, 1])


def solution(mesh):
    placed = (
        P(("dp", "fsdp"), None),
        P(("dp", "fsdp"), None),
        P(("dp", "fsdp")),
        P(("dp", "fsdp"), None),
        P("fsdp", None),
        P("fsdp", None),
        P("fsdp"),
        P("fsdp"),
    )
    return jax.shard_map(
        per_device,
        mesh=mesh,
        in_specs=placed,
        out_specs=(P(("dp", "fsdp"), None), P("fsdp", None), P("fsdp", None), P("fsdp"), P("fsdp")),
        check_vma=False,
    )
```
